32 devices in a mesh: seq: 32 (over z, y, x, core).
Axes of the slice: x: 2, y: 2, z: 4, core: 2. Of those that a mesh axis runs over, the one named last changes fastest.
Arguments:
- query: bfloat16 [32, 64, 128], replicated, may hold values from -8 to 8
- k_cache: bfloat16 [32, 6144, 1024], P(None, 'seq'), may hold values from -8 to 8
- v_cache: bfloat16 [32, 6144, 1024], P(None, 'seq'), may hold values from -16 to 16
- lengths: int32 [32], replicated, may hold values from 1 to 6144, as said below
Outputs:
- attended: float32 [2048, 128], P('seq')
The draws below stay inside these ranges and needn't reach their ends.
Inputs may be any that keep to these rules, and one draw needn't show every extreme that they name: `lengths`: every length is between 1 and 6144; some sequence has length 6144 and some has length 1.
All inputs are finite; a program needn't handle non-finite values.
Results may differ from the reference program's by a relative error of at most 0.0028.
Values sent between devices are 32-bit elements.
A program may use at most 128 MiB of HBM per device.

```python
import jax
import jax.numpy as jnp
from jax import lax

SEQS = 32
KV_DEV = 192
HQ = 64
KVH = 8
HD = 128
GROUP = 8
CTX = 6144


def draw_query(key, part):
    values = jax.random.uniform(jax.random.fold_in(key, 3), (SEQS, HQ, HD), jnp.float32, -8.0, 8.0)
    return values.astype(jnp.bfloat16)


def draw_k_cache(key, part):
    shards = CTX // KV_DEV
    columns = KVH * HD
    shared = jax.random.normal(jax.random.fold_in(key, 1), (SEQS, shards, 1, columns), jnp.float32)
    noise = jax.random.normal(jax.random.fold_in(key, 2), (SEQS, shards, KV_DEV, columns), jnp.float32)
    values = jnp.clip(shared + noise, -8.0, 8.0).reshape(SEQS, CTX, columns)
    return values.astype(jnp.bfloat16)


def draw_v_cache(key, part):
    shards = CTX // KV_DEV
    columns = KVH * HD
    shared = 3.0 * jax.random.normal(jax.random.fold_in(key, 4), (SEQS, shards, 1, columns), jnp.float32)
    noise = jax.random.normal(jax.random.fold_in(key, 5), (SEQS, shards, KV_DEV, columns), jnp.float32)
    values = jnp.clip(shared + noise, -16.0, 16.0).reshape(SEQS, CTX, columns)
    return values.astype(jnp.bfloat16)


def draw_lengths(key, part):
    drawn = jax.random.randint(jax.random.fold_in(key, 6), (SEQS,), 1, CTX + 1, dtype=jnp.int32)
    picked = jax.random.randint(jax.random.fold_in(key, 7), (), 0, SEQS, dtype=jnp.int32)
    index = lax.broadcasted_iota(jnp.int32, (SEQS,), 0)
    drawn = jnp.where(index == (picked + 1) % SEQS, 1, drawn)
    drawn = jnp.where(index == picked, CTX, drawn)
    return drawn.astype(jnp.int32)


def setup_inputs(seed: int = 0) -> dict:
    key_list = jax.random.split(jax.random.key(seed), 5)
    query = draw_query(jax.random.fold_in(key_list[4], 71), 0)
    k_cache = draw_k_cache(jax.random.fold_in(key_list[4], 71), 0)
    v_cache = draw_v_cache(jax.random.fold_in(key_list[4], 71), 0)
    lengths = draw_lengths(jax.random.fold_in(key_list[4], 71), 0)
    return {"query": query, "k_cache": k_cache, "v_cache": v_cache, "lengths": lengths}


masked_floor = -1.0e30


def reference(query, k_cache, v_cache, lengths):
    def one_sequence(items):
        row_query, row_keys, row_values, length = items
        grouped = row_query.reshape(KVH, GROUP, HD).astype(jnp.float32)
        keys = row_keys.reshape(CTX, KVH, HD).astype(jnp.float32)
        values = row_values.reshape(CTX, KVH, HD).astype(jnp.float32)
        scores = jnp.einsum("kgd,pkd->kgp", grouped, keys, precision=lax.Precision.HIGHEST) * (HD ** -0.5)
        positions = lax.broadcasted_iota(jnp.int32, (1, 1, CTX), 2)
        valid = positions < length
        scores = jnp.where(valid, scores, masked_floor)
        highest = jnp.max(scores, axis=2, keepdims=True)
        weights = jnp.where(valid, jnp.exp(scores - highest), 0.0)
        denom = jnp.sum(weights, axis=2)
        rounded = lax.optimization_barrier(weights.astype(jnp.bfloat16)).astype(jnp.float32)
        numer = jnp.einsum("kgp,pkd->kgd", rounded, values, precision=lax.Precision.HIGHEST)
        return (numer / denom[..., None]).reshape(KVH * GROUP, HD)

    result = lax.map(one_sequence, (query, k_cache, v_cache, lengths))
    return result.reshape(SEQS * HQ, HD)
```

```python
import functools

import jax
import jax.numpy as jnp
from jax import lax
from jax.experimental import pallas as pl
from jax.experimental.pallas import tpu as pltpu
from jax.sharding import PartitionSpec as P

masked_floor = -1e30
LEAD = 3
BLOCK = 2
DELAY = 1


def low_bit(j):
    return j & -j


def merge_order(count):
    order = []
    step = 2
    while step < count:
        order += [d for d in range(count - 1, 0, -1) if low_bit(d) == step]
        step *= 2
    return order + [0]


def plan(count):
    evens = merge_order(count)
    odds = [d + 1 for d in evens]
    computes = odds[:LEAD]
    for i, d in enumerate(evens):
        if i + LEAD < len(odds):
            computes.append(odds[i + LEAD])
        computes.append(d)
    blocks = [computes[i : i + BLOCK] for i in range(0, len(computes), BLOCK)]
    merges = [[] for _ in range(len(blocks) + DELAY)]
    for i, block in enumerate(blocks):
        merges[i + DELAY] += [d for d in block if d % 2 == 0 and d != 0]
    return blocks, merges


def kernel(
    devices, kv_heads, final,
    lengths_ref, q_hbm, k_hbm, v_hbm, out_ref,
    qbuf, kbuf, vbuf, acc, got,
    q_sem, k_sem, v_sem, send_sem, recv_sem,
):
    sequences, heads, head_size = qbuf.shape
    positions = kbuf.shape[1]
    group = heads // kv_heads
    me = lax.axis_index("seq")
    spread = devices // sequences
    mine = me // spread
    rest = me % spread
    bits = sequences.bit_length() - 1

    def target(d):
        total = 0
        for k in range(bits):
            bit = (mine // (1 << k)) % 2
            if d >> k & 1:
                bit = 1 - bit
            total = total + bit * (1 << k)
        return total

    barrier = pltpu.get_barrier_semaphore()
    partners = [target(1 << k) * spread + rest for k in range(bits)]
    blocks, merges = plan(sequences)

    copies = {}
    q_copy = pltpu.make_async_copy(q_hbm, qbuf, q_sem)
    q_copy.start()
    for block in blocks:
        for d in block:
            t = target(d)
            copies[d] = (
                pltpu.make_async_copy(k_hbm.at[t], kbuf.at[d], k_sem.at[d]),
                pltpu.make_async_copy(v_hbm.at[t], vbuf.at[d], v_sem.at[d]),
            )
            copies[d][0].start()
            copies[d][1].start()
    for partner in partners:
        pl.semaphore_signal(
            barrier, inc=1, device_id=(partner,), device_id_type=pl.DeviceIdType.MESH
        )
    q_copy.wait()

    lane = lax.broadcasted_iota(jnp.int32, (group, 128), 1)
    row = lax.broadcasted_iota(jnp.int32, (2 * group, head_size), 0)
    upper = jnp.where(row < group, 1.0, 0.0).astype(jnp.bfloat16)
    lower = jnp.where(row < group, 0.0, 1.0).astype(jnp.bfloat16)
    where_at = me * positions + lax.broadcasted_iota(jnp.int32, (2 * group, positions), 1)
    scale = head_size ** (-0.5)

    def compute(d):
        t = target(d)
        length = lengths_ref[t]
        valid = where_at < length
        stat = jnp.zeros((group, 128), jnp.float32)
        scores = []
        for j in range(kv_heads // 2):
            q = qbuf[t, pl.ds(2 * group * j, 2 * group), :]
            paired = jnp.concatenate([q * upper, q * lower], axis=1)
            scores.append(
                lax.dot_general(
                    paired,
                    kbuf[d, :, pl.ds(2 * head_size * j, 2 * head_size)],
                    (((1,), (1,)), ((), ())),
                    preferred_element_type=jnp.float32,
                )
            )
        for j in range(kv_heads // 2):
            score = jnp.where(valid, scores[j] * scale, masked_floor)
            peak = jnp.max(score, axis=1, keepdims=True)
            weight = jnp.where(valid, jnp.exp(score - peak), 0.0)
            total = jnp.sum(weight, axis=1, keepdims=True)
            result = jnp.dot(
                weight.astype(jnp.bfloat16),
                vbuf[d, :, pl.ds(2 * head_size * j, 2 * head_size)],
                preferred_element_type=jnp.float32,
            )
            for u in range(2):
                k = 2 * j + u
                rows = slice(group * u, group * (u + 1))
                acc[d, pl.ds(group * k, group), :] = result[rows, head_size * u : head_size * (u + 1)]
                stat = jnp.where(lane == k, peak[rows], stat)
                stat = jnp.where(lane == kv_heads + k, total[rows], stat)
        acc[d, pl.ds(heads, group), :] = stat

    def sending(d):
        k = low_bit(d).bit_length() - 1
        return pltpu.make_async_remote_copy(
            src_ref=acc.at[d],
            dst_ref=got.at[d],
            send_sem=send_sem.at[d],
            recv_sem=recv_sem.at[d],
            device_id=(partners[k],),
            device_id_type=pl.DeviceIdType.MESH,
        )

    def sources(d):
        limit = low_bit(d) if d else sequences
        found, step = [], 1
        while step < limit:
            found.append(d + step)
            step *= 2
        return found

    def merged(d, others):
        stats = [acc[d, pl.ds(heads, group), :]] + [got[j, pl.ds(heads, group), :] for j in others]
        top = functools.reduce(jnp.maximum, stats)
        factors = [jnp.exp(s - top) for s in stats]
        total = sum(s * pltpu.roll(f, kv_heads, 1) for s, f in zip(stats, factors))
        stat = jnp.where(lane < kv_heads, top, total)
        parts = []
        for k in range(kv_heads):
            rows = pl.ds(group * k, group)
            values = [acc[d, rows, :]] + [got[j, rows, :] for j in others]
            parts.append(sum(v * f[:, k : k + 1] for v, f in zip(values, factors)))
        return parts, stat

    def merge(d, others):
        parts, stat = merged(d, others)
        for k in range(kv_heads):
            acc[d, pl.ds(group * k, group), :] = parts[k]
        acc[d, pl.ds(heads, group), :] = stat

    first = True
    for i in range(len(merges)):
        block = blocks[i] if i < len(blocks) else []
        for d in block:
            copies[d][0].wait()
            copies[d][1].wait()
        for d in merges[i]:
            for j in sources(d):
                sending(j).wait_recv()
        for d in block:
            compute(d)
        for d in merges[i]:
            merge(d, sources(d))
        if first:
            pl.semaphore_wait(barrier, bits)
            first = False
        for d in merges[i] + [d for d in block if d % 2]:
            sending(d).start()

    early, late = sources(0)[:-2], sources(0)[-2:]
    for j in early:
        sending(j).wait_recv()
    merge(0, early)
    for j in late:
        sending(j).wait_recv()
    parts, stat = merged(0, late)
    for k in range(kv_heads):
        if final:
            parts[k] = parts[k] / stat[:, kv_heads + k : kv_heads + k + 1]
        out_ref[pl.ds(group * k, group), :] = parts[k]
    if not final:
        out_ref[pl.ds(heads, group), :] = stat
    for d in range(1, sequences):
        sending(d).wait_send()


def body(devices, query, k_cache, v_cache, lengths):
    sequences, heads, head_size = query.shape
    positions, columns = k_cache.shape[1:]
    kv_heads = columns // head_size
    group = heads // kv_heads
    spread = devices // sequences
    final = spread == 1
    rows = heads if final else heads + group
    anywhere = pl.BlockSpec(memory_space=pl.ANY)
    out = pl.pallas_call(
        functools.partial(kernel, devices, kv_heads, final),
        out_shape=jax.ShapeDtypeStruct((rows, head_size), jnp.float32),
        in_specs=[pl.BlockSpec(memory_space=pltpu.SMEM), anywhere, anywhere, anywhere],
        out_specs=pl.BlockSpec(memory_space=pltpu.VMEM),
        scratch_shapes=[
            pltpu.VMEM(query.shape, query.dtype),
            pltpu.VMEM(k_cache.shape, k_cache.dtype),
            pltpu.VMEM(v_cache.shape, v_cache.dtype),
            pltpu.VMEM((sequences, heads + group, head_size), jnp.float32),
            pltpu.VMEM((sequences, heads + group, head_size), jnp.float32),
            pltpu.SemaphoreType.DMA,
            pltpu.SemaphoreType.DMA((sequences,)),
            pltpu.SemaphoreType.DMA((sequences,)),
            pltpu.SemaphoreType.DMA((sequences,)),
            pltpu.SemaphoreType.DMA((sequences,)),
        ],
        compiler_params=pltpu.CompilerParams(
            collective_id=0, has_side_effects=True, vmem_limit_bytes=56 * 1024 * 1024
        ),
    )(lengths, query, k_cache, v_cache)
    if final:
        return out
    share = heads // spread
    rest = lax.axis_index("seq") % spread
    weighted = out[:heads]
    peak = out[heads:, :kv_heads].T.reshape(heads, 1)
    total = out[heads:, kv_heads : 2 * kv_heads].T.reshape(heads, 1)
    packed = jnp.concatenate([weighted, peak, total], axis=1)
    pieces = []
    for shift in range(spread):
        piece = lax.dynamic_slice_in_dim(packed, (rest + shift) % spread * share, share, 0)
        if shift:
            moves = [(i, i // spread * spread + (i + shift) % spread) for i in range(devices)]
            piece = lax.ppermute(piece, "seq", moves)
        pieces.append(piece)
    pieces = jnp.stack(pieces)
    factor = jnp.exp(pieces[:, :, head_size] - jnp.max(pieces[:, :, head_size], axis=0))
    denom = jnp.sum(pieces[:, :, head_size + 1] * factor, axis=0)
    numer = jnp.sum(pieces[:, :, :head_size] * factor[:, :, None], axis=0)
    return numer / denom[:, None]


def solution(mesh):
    placed = (P(), P(None, "seq", None), P(None, "seq", None), P())
    return jax.shard_map(
        functools.partial(body, mesh.shape["seq"]),
        mesh=mesh, in_specs=placed, out_specs=P("seq", None), check_vma=False,
    )
```

```python
import functools

import jax
import jax.numpy as jnp
from jax import lax
from jax.experimental import pallas as pl
from jax.experimental.pallas import tpu as pltpu
from jax.sharding import PartitionSpec as P

masked_floor = -1e30
LEAD = 3
BLOCK = 4
DELAY = 0
HOP = 4
LATE = True
EARLY = 4
AHEAD = 8


def stages(count):
    bits = count.bit_length() - 1
    found, low = [(0, 1)], 1
    while low < bits:
        size = min(2, bits - low)
        found.append((low, size))
        low += size
    return found


def digits(d, count):
    return [(low, d >> low & ((1 << size) - 1)) for low, size in stages(count)]


def hop(d, count):
    low, value = next(pair for pair in digits(d, count) if pair[1])
    return value << low


def sources(d, count):
    found = []
    for low, size in stages(count):
        if d >> low & ((1 << size) - 1):
            break
        found += [d + (value << low) for value in range(1, 1 << size)]
    return found


def merge_order(count):
    waiting = list(range(count - 2, 0, -2))
    ready, order = {}, []

    def when(d):
        return max([ready.get(j, 99) for j in sources(d, count) if j % 2 == 0] or [-99])

    while waiting:
        free = [d for d in waiting if when(d) + HOP <= len(order)] or [min(waiting, key=when)]
        pick = max(free, key=lambda d: (sum(value > 0 for _, value in digits(d, count)), d))
        ready[pick] = len(order)
        order.append(pick)
        waiting.remove(pick)
    return order + [0]


def plan(count):
    evens = merge_order(count)
    odds = [d + 1 for d in evens]
    computes = odds[:LEAD]
    for i, d in enumerate(evens):
        if i + LEAD < len(odds):
            computes.append(odds[i + LEAD])
        computes.append(d)
    blocks = [computes[i : i + BLOCK] for i in range(0, len(computes), BLOCK)]
    merges = [[] for _ in range(len(blocks) + DELAY)]
    for i, block in enumerate(blocks):
        merges[i + DELAY] += [d for d in block if d % 2 == 0 and d != 0]
    return blocks, merges


def kernel(
    devices, kv_heads, final,
    lengths_ref, q_hbm, k_hbm, v_hbm, out_ref,
    qbuf, kbuf, vbuf, acc, got,
    q_sem, k_sem, v_sem, send_sem, recv_sem,
):
    sequences, heads, head_size = qbuf.shape
    positions = kbuf.shape[1]
    group = heads // kv_heads
    me = lax.axis_index("seq")
    spread = devices // sequences
    mine = me // spread
    rest = me % spread
    bits = sequences.bit_length() - 1

    own = [(mine // (1 << k)) % 2 for k in range(bits)]

    def target(d):
        return sum((own[k] + (d >> k & 1)) % 2 * (1 << k) for k in range(bits))

    barrier = pltpu.get_barrier_semaphore()
    steps = [value << low for low, size in stages(sequences) for value in range(1, 1 << size)]
    partners = [target(step) * spread + rest for step in steps]
    blocks, merges = plan(sequences)

    copies = {}
    q_copy = pltpu.make_async_copy(q_hbm, qbuf, q_sem)
    q_copy.start()
    for block in blocks:
        for d in block:
            t = target(d)
            copies[d] = (
                pltpu.make_async_copy(k_hbm.at[t], kbuf.at[d], k_sem.at[d]),
                pltpu.make_async_copy(v_hbm.at[t], vbuf.at[d], v_sem.at[d]),
            )
    order = [d for block in blocks for d in block]

    def fetch(places):
        for d in order[places]:
            copies[d][0].start()
            copies[d][1].start()

    fetch(slice(0, AHEAD))
    for partner in partners:
        pl.semaphore_signal(
            barrier, inc=1, device_id=(partner,), device_id_type=pl.DeviceIdType.MESH
        )
    q_copy.wait()

    lane = lax.broadcasted_iota(jnp.int32, (group, 128), 1)
    row = lax.broadcasted_iota(jnp.int32, (2 * group, head_size), 0)
    upper = jnp.where(row < group, 1.0, 0.0).astype(jnp.bfloat16)
    lower = jnp.where(row < group, 0.0, 1.0).astype(jnp.bfloat16)
    where_at = me * positions + lax.broadcasted_iota(jnp.int32, (2 * group, positions), 1)
    scale = head_size ** (-0.5)

    def compute(d):
        t = target(d)
        length = lengths_ref[t]
        valid = where_at < length
        stat = jnp.zeros((group, 128), jnp.float32)
        scores = []
        for j in range(kv_heads // 2):
            q = qbuf[t, pl.ds(2 * group * j, 2 * group), :]
            paired = jnp.concatenate([q * upper, q * lower], axis=1)
            scores.append(
                lax.dot_general(
                    paired,
                    kbuf[d, :, pl.ds(2 * head_size * j, 2 * head_size)],
                    (((1,), (1,)), ((), ())),
                    preferred_element_type=jnp.float32,
                )
            )
        for j in range(kv_heads // 2):
            score = jnp.where(valid, scores[j] * scale, masked_floor)
            peak = jnp.max(score, axis=1, keepdims=True)
            weight = jnp.where(valid, jnp.exp(score - peak), 0.0)
            total = jnp.sum(weight, axis=1, keepdims=True)
            result = jnp.dot(
                weight.astype(jnp.bfloat16),
                vbuf[d, :, pl.ds(2 * head_size * j, 2 * head_size)],
                preferred_element_type=jnp.float32,
            )
            for u in range(2):
                k = 2 * j + u
                rows = slice(group * u, group * (u + 1))
                acc[d, pl.ds(group * k, group), :] = result[rows, head_size * u : head_size * (u + 1)]
                stat = jnp.where(lane == k, peak[rows], stat)
                stat = jnp.where(lane == kv_heads + k, total[rows], stat)
        acc[d, pl.ds(heads, group), :] = stat

    def sending(d):
        return pltpu.make_async_remote_copy(
            src_ref=acc.at[d],
            dst_ref=got.at[d],
            send_sem=send_sem.at[d],
            recv_sem=recv_sem.at[d],
            device_id=(target(hop(d, sequences)) * spread + rest,),
            device_id_type=pl.DeviceIdType.MESH,
        )

    def merged(d, others):
        stats = [acc[d, pl.ds(heads, group), :]] + [got[j, pl.ds(heads, group), :] for j in others]
        top = functools.reduce(jnp.maximum, stats)
        factors = [jnp.exp(s - top) for s in stats]
        total = sum(s * pltpu.roll(f, kv_heads, 1) for s, f in zip(stats, factors))
        stat = jnp.where(lane < kv_heads, top, total)
        parts = []
        for k in range(kv_heads):
            rows = pl.ds(group * k, group)
            values = [acc[d, rows, :]] + [got[j, rows, :] for j in others]
            parts.append(sum(v * f[:, k : k + 1] for v, f in zip(values, factors)))
        return parts, stat

    def merge(d, others):
        parts, stat = merged(d, others)
        for k in range(kv_heads):
            acc[d, pl.ds(group * k, group), :] = parts[k]
        acc[d, pl.ds(heads, group), :] = stat

    first = True
    for i in range(len(merges)):
        block = blocks[i] if i < len(blocks) else []
        for d in block:
            copies[d][0].wait()
            copies[d][1].wait()
        fetch(slice(i * BLOCK + AHEAD, (i + 1) * BLOCK + AHEAD))
        if LATE:
            for d in block:
                compute(d)
            if first:
                pl.semaphore_wait(barrier, len(partners))
                first = False
            for d in block:
                if d % 2:
                    sending(d).start()
        for d in merges[i]:
            for j in sources(d, sequences):
                sending(j).wait_recv()
        if not LATE:
            for d in block:
                compute(d)
        for d in merges[i]:
            merge(d, sources(d, sequences))
        if first:
            pl.semaphore_wait(barrier, len(partners))
            first = False
        for d in merges[i] + [d for d in block if d % 2 and not LATE]:
            sending(d).start()

    others = sources(0, sequences)
    early, late = others[:EARLY], others[EARLY:]
    for j in early:
        sending(j).wait_recv()
    merge(0, early)
    for j in late:
        sending(j).wait_recv()
    parts, stat = merged(0, late)
    for k in range(kv_heads):
        if final:
            parts[k] = parts[k] / stat[:, kv_heads + k : kv_heads + k + 1]
        out_ref[pl.ds(group * k, group), :] = parts[k]
    if not final:
        out_ref[pl.ds(heads, group), :] = stat
    for d in range(1, sequences):
        sending(d).wait_send()


def body(devices, query, k_cache, v_cache, lengths):
    sequences, heads, head_size = query.shape
    positions, columns = k_cache.shape[1:]
    kv_heads = columns // head_size
    group = heads // kv_heads
    spread = devices // sequences
    final = spread == 1
    rows = heads if final else heads + group
    anywhere = pl.BlockSpec(memory_space=pl.ANY)
    out = pl.pallas_call(
        functools.partial(kernel, devices, kv_heads, final),
        out_shape=jax.ShapeDtypeStruct((rows, head_size), jnp.float32),
        in_specs=[pl.BlockSpec(memory_space=pltpu.SMEM), anywhere, anywhere, anywhere],
        out_specs=pl.BlockSpec(memory_space=pltpu.VMEM),
        scratch_shapes=[
            pltpu.VMEM(query.shape, query.dtype),
            pltpu.VMEM(k_cache.shape, k_cache.dtype),
            pltpu.VMEM(v_cache.shape, v_cache.dtype),
            pltpu.VMEM((sequences, heads + group, head_size), jnp.float32),
            pltpu.VMEM((sequences, heads + group, head_size), jnp.float32),
            pltpu.SemaphoreType.DMA,
            pltpu.SemaphoreType.DMA((sequences,)),
            pltpu.SemaphoreType.DMA((sequences,)),
            pltpu.SemaphoreType.DMA((sequences,)),
            pltpu.SemaphoreType.DMA((sequences,)),
        ],
        compiler_params=pltpu.CompilerParams(
            collective_id=0, has_side_effects=True, vmem_limit_bytes=56 * 1024 * 1024
        ),
    )(lengths, query, k_cache, v_cache)
    if final:
        return out
    share = heads // spread
    rest = lax.axis_index("seq") % spread
    weighted = out[:heads]
    peak = out[heads:, :kv_heads].T.reshape(heads, 1)
    total = out[heads:, kv_heads : 2 * kv_heads].T.reshape(heads, 1)
    packed = jnp.concatenate([weighted, peak, total], axis=1)
    pieces = []
    for shift in range(spread):
        piece = lax.dynamic_slice_in_dim(packed, (rest + shift) % spread * share, share, 0)
        if shift:
            moves = [(i, i // spread * spread + (i + shift) % spread) for i in range(devices)]
            piece = lax.ppermute(piece, "seq", moves)
        pieces.append(piece)
    pieces = jnp.stack(pieces)
    factor = jnp.exp(pieces[:, :, head_size] - jnp.max(pieces[:, :, head_size], axis=0))
    denom = jnp.sum(pieces[:, :, head_size + 1] * factor, axis=0)
    numer = jnp.sum(pieces[:, :, :head_size] * factor[:, :, None], axis=0)
    return numer / denom[:, None]


def solution(mesh):
    placed = (P(), P(None, "seq", None), P(None, "seq", None), P())
    return jax.shard_map(
        functools.partial(body, mesh.shape["seq"]),
        mesh=mesh, in_specs=placed, out_specs=P("seq", None), check_vma=False,
    )
```
